32 devices in a mesh: level: 2 (over core), gx: 4 (over y, x), yz: 4 (over z).
Axes of the slice: x: 2, y: 2, z: 4, core: 2. Of those that a mesh axis runs over, the one named last changes fastest.
Arguments:
- init_field: float32 [128, 64, 256], P('gx', 'yz'), may hold values from -6 to 6
- source: float32 [128, 64, 256], P('gx', 'yz'), may hold values from -4 to 4
- damping: float32 [128, 64, 256], P('gx', 'yz'), may hold values from 0.05 to 2
Outputs:
- final_states: float32 [2, 128, 64, 256], P('level', 'gx', 'yz')
The draws below stay inside these ranges and needn't reach their ends.
All inputs are finite; a program needn't handle non-finite values.
Results may differ from the reference program's by a relative error of at most 0.0001.
Values sent between devices are 32-bit elements; how exact they have to be, the bound alone decides.
A program may use at most 64 MiB of HBM per device.

```python
import math
import jax
import jax.numpy as jnp

STEPS = 3
ITERS = 3
NX = 128
NY = 64
NZ = 256


def block_scale(rng, extent, split, low, high):
    level, own = 1.0, jax.random.fold_in(rng, 6)
    for position, parts in split:
        steps = jnp.exp(jax.random.uniform(jax.random.fold_in(own, position), (parts,), jnp.float32, low / len(split), high / len(split)))
        level = level * jnp.repeat(steps, extent[position] // parts).reshape([-1 if axis == position else 1 for axis in range(len(extent))])
    return level


def noise(stream_key, shape, deviation, most, shards=(), dtype=jnp.bfloat16):
    gain = block_scale(stream_key, shape, shards, -0.22, 0.18) if shards else 1.0
    array = jax.random.normal(stream_key, shape, jnp.float32) * deviation * gain
    return jnp.minimum(jnp.maximum(array, -most), most).astype(dtype)


def setup_inputs(seed: int = 0) -> dict:
    keys = jax.random.split(jax.random.key(seed), 4)
    init_field = noise(keys[0], (NX, NY, NZ), 1.0, 6.0, ((0, 4), (1, 4)), jnp.float32)
    source = noise(keys[1], (NX, NY, NZ), 0.5, 4.0, ((0, 4), (1, 4)), jnp.float32)
    damping = jnp.clip(jnp.exp(math.log(2.0) - 3.6888794 * jax.random.uniform(keys[2], (NX, NY, NZ), jnp.float32) ** block_scale(keys[2], (NX, NY, NZ), ((0, 4), (1, 4)), -0.2, 0.2)), 0.05, 2.0)
    return dict(init_field=init_field, source=source, damping=damping)


diffusion_number = 1.0


def stencil(field, damping):
    padded = jnp.pad(field, 1)
    beside = padded[2:, 1:-1, 1:-1] + padded[:-2, 1:-1, 1:-1]
    beside = beside + padded[1:-1, 2:, 1:-1] + padded[1:-1, :-2, 1:-1]
    beside = beside + padded[1:-1, 1:-1, 2:] + padded[1:-1, 1:-1, :-2]
    return damping * field + diffusion_number * (6.0 * field - beside)


def solve(target, guess, damping):
    answer = guess
    resid = target - (answer + stencil(answer, damping))
    direction = resid
    norm_now = jnp.sum(resid * resid)
    for step in range(ITERS):
        image = direction + stencil(direction, damping)
        alpha = norm_now / jnp.sum(direction * image)
        answer = answer + alpha * direction
        resid = resid - alpha * image
        if step + 1 < ITERS:
            norm_next = jnp.sum(resid * resid)
            direction = resid + (norm_next / norm_now) * direction
            norm_now = norm_next
    return answer


def reference(init_field, source, damping):
    states = [init_field]
    for step in range(STEPS):
        states.append(solve(states[-1] + source, states[-1], damping))
    corrected = init_field
    for step in range(STEPS):
        extra = 0.5 * stencil(states[step + 1] - states[step], damping)
        corrected = solve(corrected + source + extra, corrected, damping)
    return jnp.stack([states[-1], corrected])
```

```python
import functools

import jax
import jax.numpy as jnp
from jax import lax
from jax.experimental import pallas as pl
from jax.experimental.pallas import tpu as pltpu
from jax.sharding import PartitionSpec as P

STEPS = 3
ITERS = 3
PX = 3
PY = 8
LANES = 128
MID = 8.025
HALF = 6.975
MESH = pl.DeviceIdType.MESH
DIRS = ((-1, 0), (1, 0), (0, -1), (0, 1), (-1, -1), (-1, 1), (1, -1), (1, 1))


def times_a(c):
    out = [MID * v for v in c] + [jnp.zeros_like(c[0])]
    for k, v in enumerate(c):
        if k == 0:
            out[1] = out[1] + HALF * v
        else:
            out[k + 1] = out[k + 1] + (0.5 * HALF) * v
            out[k - 1] = out[k - 1] + (0.5 * HALF) * v
    return out


def plus(a, b):
    short, long = (a, b) if len(a) < len(b) else (b, a)
    return [x + y for x, y in zip(short, long)] + long[len(short):]


def scaled(s, a):
    return [s * x for x in a]


def cg_coefficients(dots):
    m = [dots[0], dots[1], 2.0 * dots[2] - dots[0], 2.0 * dots[3] - dots[1],
         2.0 * dots[4] - dots[0], 2.0 * dots[5] - dots[1]]

    def inner(a, b):
        total = None
        for i, x in enumerate(a):
            for j, y in enumerate(b):
                term = (x * y) * (0.5 * (m[i + j] + m[abs(i - j)]))
                total = term if total is None else total + term
        return total

    one = jnp.ones_like(m[0])
    resid = [one]
    direction = resid
    image = times_a(resid)
    along = image
    norm_now = m[0]
    alpha = norm_now / inner(resid, image)
    answer = None
    for step in range(ITERS):
        move = scaled(alpha, direction)
        answer = move if answer is None else plus(answer, move)
        if step + 1 < ITERS:
            resid = plus(resid, scaled(-alpha, along))
            image = times_a(resid)
            norm_next = inner(resid, resid)
            product = inner(resid, image)
            ratio = norm_next / norm_now
            alpha = norm_next / (product - ratio * norm_next / alpha)
            direction = plus(resid, scaled(ratio, direction))
            along = plus(image, scaled(ratio, along))
            norm_now = norm_next
    change = plus(times_a(answer), scaled(-1.0, answer))
    return answer, change


def body(sizes, stages, init_ref, source_ref, damp_ref, out_ref, p0, src, dmp, heads_p, heads_c,
         work_p, work_c, base, sums, result, slots, in_sem, send_sem, recv_sem, red_send, red_recv, out_sem):
    levels, nx, ny = sizes
    half = src.shape[0]
    parts = src.shape[1]
    rows = src.shape[2]
    level, gx, yz = lax.axis_index("level"), lax.axis_index("gx"), lax.axis_index("yz")
    xpos = gx * levels + level
    xcount = nx * levels
    x_in = (xpos > 0, xpos < xcount - 1)
    y_in = (yz > 0, yz < ny - 1)

    def exists(dx, dy):
        ok = None
        for d, pair in ((dx, x_in), (dy, y_in)):
            if d != 0:
                c = pair[0] if d < 0 else pair[1]
                ok = c if ok is None else jnp.logical_and(ok, c)
        return ok

    mine = pl.ds(level * half, half)
    loads = []
    for i, (ref, buf, pad) in enumerate(((init_ref, p0, True), (damp_ref, dmp, True), (source_ref, src, False))):
        for z in range(parts):
            lanes = slice(z * LANES, (z + 1) * LANES)
            dst = buf.at[PX:PX + half, z, PY:PY + rows, :] if pad else buf.at[:, z, :, :]
            copy = pltpu.make_async_copy(ref.at[mine, :, lanes], dst, in_sem.at[i, z])
            copy.start()
            loads.append(copy)

    zero_x = jnp.zeros((PX,) + tuple(p0.shape[1:]), jnp.float32)
    zero_y = jnp.zeros((p0.shape[0], parts, PY, LANES), jnp.float32)
    for buf in [p0] + [h.at[n] for h in (heads_p, heads_c) for n in range(STEPS)]:
        @pl.when(jnp.logical_not(x_in[0]))
        def _(buf=buf):
            buf[0:PX] = zero_x

        @pl.when(jnp.logical_not(x_in[1]))
        def _(buf=buf):
            buf[PX + half:] = zero_x

        @pl.when(jnp.logical_not(y_in[0]))
        def _(buf=buf):
            buf[:, :, 0:PY, :] = zero_y

        @pl.when(jnp.logical_not(y_in[1]))
        def _(buf=buf):
            buf[:, :, PY + rows:, :] = zero_y

    def halo_copy(buf, width, slot, k):
        dx, dy = DIRS[k]
        w = width if 0 in (dx, dy) else width - 1
        if w == 0:
            return None

        def spans(d, pad, size):
            if d == 0:
                return slice(pad, pad + size), slice(pad, pad + size)
            if d < 0:
                return slice(pad, pad + w), slice(pad + size, pad + size + w)
            return slice(pad + size - w, pad + size), slice(pad - w, pad)

        sx, tx = spans(dx, PX, half)
        sy, ty = spans(dy, PY, rows)
        to = xpos + dx
        return pltpu.make_async_remote_copy(
            src_ref=buf.at[sx, :, sy, :], dst_ref=buf.at[tx, :, ty, :],
            send_sem=send_sem.at[slot, k], recv_sem=recv_sem.at[slot, k],
            device_id={"level": lax.rem(to + levels, levels), "gx": lax.div(to + levels, levels) - 1, "yz": yz + dy},
            device_id_type=MESH,
        )

    order = (4, 5, 6, 7, 2, 3, 0, 1)

    def send_halo(buf, width, slot):
        for k in order:
            copy = halo_copy(buf, width, slot, k)
            if copy is not None:
                pl.when(exists(*DIRS[k]))(lambda copy=copy: copy.start())

    def wait_halo(buf, width, slot):
        for k in order:
            copy = halo_copy(buf, width, slot, k)
            if copy is not None:
                dx, dy = DIRS[k]
                pl.when(exists(-dx, -dy))(lambda copy=copy: copy.wait_recv())

    def end_halo(buf, width, slot):
        for k in order:
            copy = halo_copy(buf, width, slot, k)
            if copy is not None:
                pl.when(exists(*DIRS[k]))(lambda copy=copy: copy.wait_send())

    def stencil(v, x, start, count):
        lane = lax.broadcasted_iota(jnp.int32, (count, LANES), 1)
        own = pl.ds(start, count)
        centre = [v[x, z, own, :] for z in range(parts)]
        fore = [pltpu.roll(c, 1, 1) for c in centre]
        back = [pltpu.roll(c, LANES - 1, 1) for c in centre]
        out = []
        for z in range(parts):
            near = jnp.where(lane == 0, fore[z - 1] if z > 0 else 0.0, fore[z])
            far = jnp.where(lane == LANES - 1, back[z + 1] if z + 1 < parts else 0.0, back[z])
            beside = v[x - 1, z, own, :] + v[x + 1, z, own, :]
            beside = beside + v[x, z, pl.ds(start - 1, count), :] + v[x, z, pl.ds(start + 1, count), :]
            beside = beside + (near + far)
            out.append((dmp[x, z, own, :] + (7.0 - MID)) * centre[z] - beside)
        return out, centre

    low = jnp.where(y_in[0], 0, PY)
    high = jnp.where(y_in[1], 2 * PY + rows, PY + rows)
    first = jnp.where(x_in[0], 0, PX)
    last = jnp.where(x_in[1], 2 * PX + half, PX + half)

    def fold(block):
        return jnp.sum(block.reshape(-1, 8, LANES), axis=0)

    def powers(head, work):
        zero = jnp.zeros((8, LANES), jnp.float32)
        own = pl.ds(PY, rows)
        totals = []
        for k in range(1, ITERS + 1):
            h = ITERS - k
            start = PY - h
            count = -(-(rows + 2 * h) // 8) * 8
            prev = head if k == 1 else work.at[k - 2]
            row = lax.broadcasted_iota(jnp.int32, (count, LANES), 0) + start

            def plane(x, carry, k=k, h=h, start=start, count=count, prev=prev, row=row):
                t, centre = stencil(prev, x, start, count)
                if h > 0:
                    top = jnp.where(jnp.logical_and(x >= first, x < last), high, 0)
                    ok = jnp.logical_and(row >= low, row < top)
                for z in range(parts):
                    if k == 1:
                        new = t[z] * (1.0 / HALF)
                    else:
                        older = head if k == 2 else work.at[k - 3]
                        new = t[z] * (2.0 / HALF) - older[x, z, pl.ds(start, count), :]
                    if h > 0:
                        new = jnp.where(ok, new, 0.0)
                    work[k - 1, x, z, pl.ds(start, count), :] = new
                return carry

            def inside(x, carry, k=k, prev=prev, plane=plane):
                plane(x, 0)
                a, b = carry
                for z in range(parts):
                    v = prev[x, z, own, :]
                    w = work[k - 1, x, z, own, :]
                    a = a + fold(v * v)
                    b = b + fold(v * w)
                return a, b

            if h > 0:
                lax.fori_loop(PX - h, PX, plane, 0)
            totals += lax.fori_loop(PX, PX + half, inside, (zero, zero))
            if h > 0:
                lax.fori_loop(PX + half, PX + half + h, plane, 0)
        return totals

    def position(axes):
        flat = 0
        for a in axes:
            flat = flat * lax.axis_size(a) + lax.axis_index(a)
        return flat

    def reduce_all(accs, turn):
        n = len(accs)
        size = -(-n // 8) * 8
        eye = lax.broadcasted_iota(jnp.int32, (size, LANES), 0) == lax.broadcasted_iota(jnp.int32, (size, LANES), 1)
        tall = jnp.concatenate([jnp.sum(a, axis=0, keepdims=True) for a in accs]
                               + [jnp.zeros((size - n, LANES), jnp.float32)] * (size > n), axis=0)
        col = jnp.sum(tall, axis=1, keepdims=True)
        line = jnp.sum(jnp.where(eye, col, 0.0), axis=0, keepdims=True)
        for s, axes in enumerate(stages):
            count = 1
            for a in axes:
                count *= lax.axis_size(a)
            me = position(axes)
            cell = slots[s].at[turn, pl.ds(me, 1), :]
            cell[...] = line
            copies = []
            for off in range(1, count):
                peer = lax.rem(me + off, count)
                ids = {}
                for a in reversed(axes):
                    ids[a] = lax.rem(peer, lax.axis_size(a))
                    peer = lax.div(peer, lax.axis_size(a))
                copy = pltpu.make_async_remote_copy(
                    src_ref=cell, dst_ref=cell, send_sem=red_send[s].at[turn, off - 1],
                    recv_sem=red_recv[s].at[turn, off - 1], device_id=ids, device_id_type=MESH)
                copy.start()
                copies.append(copy)
            for copy in copies:
                copy.wait_recv()
            line = jnp.sum(slots[s][turn], axis=0, keepdims=True)
            for copy in copies:
                copy.wait_send()
        col = jnp.sum(jnp.where(eye, line, 0.0), axis=1, keepdims=True)
        wide = jnp.broadcast_to(col, (size, LANES))
        return [wide[k:k + 1, :] for k in range(n)]

    own = pl.ds(PY, rows)
    for copy in loads[:2 * parts]:
        copy.wait()
    send_halo(p0, 1, 0)
    send_halo(dmp, ITERS - 1, 1)
    for copy in loads[2 * parts:]:
        copy.wait()
    wait_halo(p0, 1, 0)

    def start_plane(x, carry):
        t, centre = stencil(p0, x, PY, rows)
        for z in range(parts):
            r = src[x - PX, z] - (t[z] + (MID - 1.0) * centre[z])
            heads_p[0, x, z, own, :] = r
            base[x - PX, z] = r
        return carry

    lax.fori_loop(PX, PX + half, start_plane, 0)

    pending = [(p0, 1, 0), (dmp, ITERS - 1, 1)]
    slot = 2
    for turn in range(STEPS + 1):
        with_p, with_c = turn < STEPS, turn > 0
        fields = []
        if with_p:
            fields.append((heads_p.at[turn], work_p))
        if with_c:
            fields.append((heads_c.at[turn - 1], work_c))
        slots_here = []
        for head, _ in fields:
            send_halo(head, ITERS, slot)
            slots_here.append((head, ITERS, slot))
            slot += 1
        if turn == 0:
            wait_halo(dmp, ITERS - 1, 1)
        accs = []
        for (head, work), item in zip(fields, slots_here):
            wait_halo(*item)
            accs += powers(head, work)
        pending += slots_here
        dots = reduce_all(accs, turn)
        coeff = [cg_coefficients(dots[6 * i:6 * i + 6]) for i in range(len(fields))]

        def update(i, carry, turn=turn, with_p=with_p, with_c=with_c, fields=fields, coeff=coeff):
            x = i + PX

            def basis(f, z):
                head, work = fields[f]
                return [head[x, z, own, :]] + [work[k, x, z, own, :] for k in range(ITERS)]

            def combine(c, v):
                total = c[0] * v[0]
                for a, b in zip(c[1:], v[1:]):
                    total = total + a * b
                return total

            for z in range(parts):
                line = base[i, z] if turn < STEPS else None
                if with_p:
                    v = basis(0, z)
                    rise = combine(coeff[0][0], v)
                    change = combine(coeff[0][1], v)
                    before = p0[x, z, own, :] if turn == 0 else sums[0, i, z]
                    if turn + 1 < STEPS:
                        sums[0, i, z] = before + rise
                        heads_p[turn + 1, x, z, own, :] = v[0] - change
                    else:
                        result[0, i, z] = before + rise
                if with_c:
                    v = basis(len(fields) - 1, z)
                    rise = combine(coeff[-1][0], v)
                    before = p0[x, z, own, :] if turn == 1 else sums[1, i, z]
                    if turn < STEPS:
                        sums[1, i, z] = before + rise
                        line = line - combine(coeff[-1][1], v)
                        base[i, z] = line
                    else:
                        result[1, i, z] = before + rise
                if turn < STEPS:
                    heads_c[turn, x, z, own, :] = line + 0.5 * change
            return carry

        lax.fori_loop(0, half, update, 0)

    ends = []
    for other in range(1, levels):
        to = lax.rem(level + other, levels)
        for z in range(parts):
            lanes = slice(z * LANES, (z + 1) * LANES)
            copy = pltpu.make_async_remote_copy(
                src_ref=result.at[to, :, z, :, :], dst_ref=out_ref.at[0, mine, :, lanes],
                send_sem=out_sem.at[0, z], recv_sem=out_sem.at[1, z],
                device_id={"level": to, "gx": gx, "yz": yz}, device_id_type=MESH)
            copy.start()
            ends.append(copy)
    for z in range(parts):
        lanes = slice(z * LANES, (z + 1) * LANES)
        copy = pltpu.make_async_copy(result.at[level, :, z, :, :], out_ref.at[0, mine, :, lanes], out_sem.at[2, z])
        copy.start()
        ends.append(copy)
    for item in pending:
        end_halo(*item)
    for copy in ends:
        copy.wait()


def solution(mesh):
    levels, nx, ny = mesh.shape["level"], mesh.shape["gx"], mesh.shape["yz"]
    if levels * nx * ny <= 64:
        stages = (("level", "gx", "yz"),)
    else:
        stages = (("level", "gx"), ("yz",))

    def per_device(init_field, source, damping):
        deep, rows, wide = init_field.shape
        half, parts = deep // levels, wide // LANES
        padded = (half + 2 * PX, parts, rows + 2 * PY, LANES)
        plain = (half, parts, rows, LANES)
        counts = []
        for axes in stages:
            n = 1
            for a in axes:
                n *= mesh.shape[a]
            counts.append(n)
        turns = STEPS + 1
        dma = pltpu.SemaphoreType.DMA
        exchanges = 2 + 2 * STEPS
        return pl.pallas_call(
            functools.partial(body, (levels, nx, ny), stages),
            out_shape=jax.ShapeDtypeStruct((1, deep, rows, wide), jnp.float32),
            in_specs=[pl.BlockSpec(memory_space=pl.ANY)] * 3,
            out_specs=pl.BlockSpec(memory_space=pl.ANY),
            scratch_shapes=[
                pltpu.VMEM(padded, jnp.float32),
                pltpu.VMEM(plain, jnp.float32),
                pltpu.VMEM(padded, jnp.float32),
                pltpu.VMEM((STEPS,) + padded, jnp.float32),
                pltpu.VMEM((STEPS,) + padded, jnp.float32),
                pltpu.VMEM((ITERS,) + padded, jnp.float32),
                pltpu.VMEM((ITERS,) + padded, jnp.float32),
                pltpu.VMEM(plain, jnp.float32),
                pltpu.VMEM((2,) + plain, jnp.float32),
                pltpu.VMEM((2,) + plain, jnp.float32),
                [pltpu.VMEM((turns, n, LANES), jnp.float32) for n in counts],
                dma((3, parts)),
                dma((exchanges, 8)),
                dma((exchanges, 8)),
                [dma((turns, n - 1)) for n in counts],
                [dma((turns, n - 1)) for n in counts],
                dma((3, parts)),
            ],
            compiler_params=pltpu.CompilerParams(has_side_effects=True),
        )(init_field, source, damping)

    spec = P("gx", "yz", None)
    return jax.shard_map(
        per_device, mesh=mesh, in_specs=(spec, spec, spec),
        out_specs=P("level", "gx", "yz", None), check_vma=False,
    )
```

```python
import functools

import jax
import jax.numpy as jnp
from jax import lax
from jax.experimental import pallas as pl
from jax.experimental.pallas import tpu as pltpu
from jax.sharding import PartitionSpec as P

STEPS = 3
ITERS = 3
PX = 3
PY = 8
LANES = 128
MID = 8.025
HALF = 6.975
MESH = pl.DeviceIdType.MESH
DIRS = ((-1, 0), (1, 0), (0, -1), (0, 1), (-1, -1), (-1, 1), (1, -1), (1, 1))


def times_a(c):
    out = [MID * v for v in c] + [jnp.zeros_like(c[0])]
    for k, v in enumerate(c):
        if k == 0:
            out[1] = out[1] + HALF * v
        else:
            out[k + 1] = out[k + 1] + (0.5 * HALF) * v
            out[k - 1] = out[k - 1] + (0.5 * HALF) * v
    return out


def plus(a, b):
    short, long = (a, b) if len(a) < len(b) else (b, a)
    return [x + y for x, y in zip(short, long)] + long[len(short):]


def scaled(s, a):
    return [s * x for x in a]


def cg_coefficients(dots):
    m = [dots[0], dots[1], 2.0 * dots[2] - dots[0], 2.0 * dots[3] - dots[1],
         2.0 * dots[4] - dots[0], 2.0 * dots[5] - dots[1]]

    def inner(a, b):
        total = None
        for i, x in enumerate(a):
            for j, y in enumerate(b):
                term = (x * y) * (0.5 * (m[i + j] + m[abs(i - j)]))
                total = term if total is None else total + term
        return total

    one = jnp.ones_like(m[0])
    resid = [one]
    direction = resid
    image = times_a(resid)
    along = image
    norm_now = m[0]
    alpha = norm_now / inner(resid, image)
    answer = None
    for step in range(ITERS):
        move = scaled(alpha, direction)
        answer = move if answer is None else plus(answer, move)
        if step + 1 < ITERS:
            resid = plus(resid, scaled(-alpha, along))
            image = times_a(resid)
            norm_next = inner(resid, resid)
            product = inner(resid, image)
            ratio = norm_next / norm_now
            alpha = norm_next / (product - ratio * norm_next / alpha)
            direction = plus(resid, scaled(ratio, direction))
            along = plus(image, scaled(ratio, along))
            norm_now = norm_next
    change = plus(times_a(answer), scaled(-1.0, answer))
    return answer, change


def body(sizes, stages, init_ref, source_ref, damp_ref, out_ref, p0, src, dmp, heads_p, heads_c,
         work_p, work_c, base, sums, result, slots, in_sem, send_sem, recv_sem, red_send, red_recv, out_sem):
    levels, nx, ny = sizes
    half = src.shape[0]
    parts = src.shape[1]
    rows = src.shape[2]
    level, gx, yz = lax.axis_index("level"), lax.axis_index("gx"), lax.axis_index("yz")
    xpos = gx * levels + level
    xcount = nx * levels
    x_in = (xpos > 0, xpos < xcount - 1)
    y_in = (yz > 0, yz < ny - 1)

    def exists(dx, dy):
        ok = None
        for d, pair in ((dx, x_in), (dy, y_in)):
            if d != 0:
                c = pair[0] if d < 0 else pair[1]
                ok = c if ok is None else jnp.logical_and(ok, c)
        return ok

    mine = pl.ds(level * half, half)
    loads = []
    for i, (ref, buf, pad) in enumerate(((init_ref, p0, True), (damp_ref, dmp, True), (source_ref, src, False))):
        for z in range(parts):
            lanes = slice(z * LANES, (z + 1) * LANES)
            dst = buf.at[PX:PX + half, z, PY:PY + rows, :] if pad else buf.at[:, z, :, :]
            copy = pltpu.make_async_copy(ref.at[mine, :, lanes], dst, in_sem.at[i, z])
            copy.start()
            loads.append(copy)

    zero_x = jnp.zeros((PX,) + tuple(p0.shape[1:]), jnp.float32)
    zero_y = jnp.zeros((p0.shape[0], parts, PY, LANES), jnp.float32)
    for buf in [p0] + [h.at[n] for h in (heads_p, heads_c) for n in range(STEPS)]:
        @pl.when(jnp.logical_not(x_in[0]))
        def _(buf=buf):
            buf[0:PX] = zero_x

        @pl.when(jnp.logical_not(x_in[1]))
        def _(buf=buf):
            buf[PX + half:] = zero_x

        @pl.when(jnp.logical_not(y_in[0]))
        def _(buf=buf):
            buf[:, :, 0:PY, :] = zero_y

        @pl.when(jnp.logical_not(y_in[1]))
        def _(buf=buf):
            buf[:, :, PY + rows:, :] = zero_y

    def halo_copy(buf, width, slot, k):
        dx, dy = DIRS[k]
        w = width if 0 in (dx, dy) else width - 1
        if w == 0:
            return None

        def spans(d, pad, size):
            if d == 0:
                return slice(pad, pad + size), slice(pad, pad + size)
            if d < 0:
                return slice(pad, pad + w), slice(pad + size, pad + size + w)
            return slice(pad + size - w, pad + size), slice(pad - w, pad)

        sx, tx = spans(dx, PX, half)
        sy, ty = spans(dy, PY, rows)
        to = xpos + dx
        return pltpu.make_async_remote_copy(
            src_ref=buf.at[sx, :, sy, :], dst_ref=buf.at[tx, :, ty, :],
            send_sem=send_sem.at[slot, k], recv_sem=recv_sem.at[slot, k],
            device_id={"level": lax.rem(to + levels, levels), "gx": lax.div(to + levels, levels) - 1, "yz": yz + dy},
            device_id_type=MESH,
        )

    order = (4, 5, 6, 7, 2, 3, 0, 1)

    def send_halo(buf, width, slot):
        for k in order:
            copy = halo_copy(buf, width, slot, k)
            if copy is not None:
                pl.when(exists(*DIRS[k]))(lambda copy=copy: copy.start())

    def wait_halo(buf, width, slot):
        for k in order:
            copy = halo_copy(buf, width, slot, k)
            if copy is not None:
                dx, dy = DIRS[k]
                pl.when(exists(-dx, -dy))(lambda copy=copy: copy.wait_recv())

    def end_halo(buf, width, slot):
        for k in order:
            copy = halo_copy(buf, width, slot, k)
            if copy is not None:
                pl.when(exists(*DIRS[k]))(lambda copy=copy: copy.wait_send())

    def stencil(v, x, start, count):
        lane = lax.broadcasted_iota(jnp.int32, (count, LANES), 1)
        own = pl.ds(start, count)
        centre = [v[x, z, own, :] for z in range(parts)]
        fore = [pltpu.roll(c, 1, 1) for c in centre]
        back = [pltpu.roll(c, LANES - 1, 1) for c in centre]
        out = []
        for z in range(parts):
            near = jnp.where(lane == 0, fore[z - 1] if z > 0 else 0.0, fore[z])
            far = jnp.where(lane == LANES - 1, back[z + 1] if z + 1 < parts else 0.0, back[z])
            beside = v[x - 1, z, own, :] + v[x + 1, z, own, :]
            beside = beside + v[x, z, pl.ds(start - 1, count), :] + v[x, z, pl.ds(start + 1, count), :]
            beside = beside + (near + far)
            out.append((dmp[x, z, own, :] + (7.0 - MID)) * centre[z] - beside)
        return out, centre

    low = jnp.where(y_in[0], 0, PY)
    high = jnp.where(y_in[1], 2 * PY + rows, PY + rows)

    def fold(block):
        return jnp.sum(block.reshape(-1, 8, LANES), axis=0)

    def powers(head, work):
        zero = jnp.zeros((8, LANES), jnp.float32)
        own = pl.ds(PY, rows)
        totals = []
        for k in range(1, ITERS + 1):
            h = ITERS - k
            start = PY - h
            count = -(-(rows + 2 * h) // 8) * 8
            prev = head if k == 1 else work.at[k - 2]
            row = lax.broadcasted_iota(jnp.int32, (count, LANES), 0) + start

            mask = jnp.logical_and(row >= low, row < high)
            keep = jnp.logical_and(row >= PY, row < PY + rows)
            older = None if k == 1 else head if k == 2 else work.at[k - 3]

            def plane(x, inner, sides, k=k, h=h, start=start, count=count, prev=prev, mask=mask, keep=keep, older=older):
                a, b = sides
                t, centre = stencil(prev, x, start, count)
                ok = mask
                if not inner:
                    ok = jnp.logical_and(mask, x_in[0] if x < PX else x_in[1])
                for z in range(parts):
                    if k == 1:
                        new = t[z] * (1.0 / HALF)
                    else:
                        new = t[z] * (2.0 / HALF) - older[x, z, pl.ds(start, count), :]
                    if h > 0:
                        new = jnp.where(ok, new, 0.0)
                    work[k - 1, x, z, pl.ds(start, count), :] = new
                    if inner:
                        square, cross = centre[z] * centre[z], centre[z] * new
                        if h > 0:
                            square, cross = jnp.where(keep, square, 0.0), jnp.where(keep, cross, 0.0)
                        a = a + fold(square)
                        b = b + fold(cross)
                return a, b

            sides = (zero, zero)
            for x in range(PX - h, PX + half + h):
                sides = plane(x, PX <= x < PX + half, sides)
            totals += sides
        return totals

    def position(axes):
        flat = 0
        for a in axes:
            flat = flat * lax.axis_size(a) + lax.axis_index(a)
        return flat

    def reduce_all(accs, turn):
        n = len(accs)
        size = -(-n // 8) * 8
        eye = lax.broadcasted_iota(jnp.int32, (size, LANES), 0) == lax.broadcasted_iota(jnp.int32, (size, LANES), 1)
        tall = jnp.concatenate([jnp.sum(a, axis=0, keepdims=True) for a in accs]
                               + [jnp.zeros((size - n, LANES), jnp.float32)] * (size > n), axis=0)
        col = jnp.sum(tall, axis=1, keepdims=True)
        line = jnp.sum(jnp.where(eye, col, 0.0), axis=0, keepdims=True)
        for s, axes in enumerate(stages):
            count = 1
            for a in axes:
                count *= lax.axis_size(a)
            me = position(axes)
            cell = slots[s].at[turn, pl.ds(me, 1), :]
            cell[...] = line
            copies = []
            for off in range(1, count):
                peer = lax.rem(me + off, count)
                ids = {}
                for a in reversed(axes):
                    ids[a] = lax.rem(peer, lax.axis_size(a))
                    peer = lax.div(peer, lax.axis_size(a))
                copy = pltpu.make_async_remote_copy(
                    src_ref=cell, dst_ref=cell, send_sem=red_send[s].at[turn, off - 1],
                    recv_sem=red_recv[s].at[turn, off - 1], device_id=ids, device_id_type=MESH)
                copy.start()
                copies.append(copy)
            for copy in copies:
                copy.wait_recv()
            line = jnp.sum(slots[s][turn], axis=0, keepdims=True)
            for copy in copies:
                copy.wait_send()
        col = jnp.sum(jnp.where(eye, line, 0.0), axis=1, keepdims=True)
        wide = jnp.broadcast_to(col, (size, LANES))
        return [wide[k:k + 1, :] for k in range(n)]

    own = pl.ds(PY, rows)
    for copy in loads[:2 * parts]:
        copy.wait()
    send_halo(p0, 1, 0)
    send_halo(dmp, ITERS - 1, 1)
    for copy in loads[2 * parts:]:
        copy.wait()
    wait_halo(p0, 1, 0)

    def start_plane(x, carry):
        t, centre = stencil(p0, x, PY, rows)
        for z in range(parts):
            r = src[x - PX, z] - (t[z] + (MID - 1.0) * centre[z])
            heads_p[0, x, z, own, :] = r
            base[x - PX, z] = r
        return carry

    lax.fori_loop(PX, PX + half, start_plane, 0)

    pending = [(p0, 1, 0), (dmp, ITERS - 1, 1)]
    slot = 2
    for turn in range(STEPS + 1):
        with_p, with_c = turn < STEPS, turn > 0
        fields = []
        if with_p:
            fields.append((heads_p.at[turn], work_p))
        if with_c:
            fields.append((heads_c.at[turn - 1], work_c))
        slots_here = []
        for head, _ in fields:
            send_halo(head, ITERS, slot)
            slots_here.append((head, ITERS, slot))
            slot += 1
        if turn == 0:
            wait_halo(dmp, ITERS - 1, 1)
        accs = []
        for (head, work), item in zip(fields, slots_here):
            wait_halo(*item)
            accs += powers(head, work)
        pending += slots_here
        dots = reduce_all(accs, turn)
        coeff = [cg_coefficients(dots[6 * i:6 * i + 6]) for i in range(len(fields))]

        def update(i, carry, turn=turn, with_p=with_p, with_c=with_c, fields=fields, coeff=coeff):
            x = i + PX

            def basis(f, z):
                head, work = fields[f]
                return [head[x, z, own, :]] + [work[k, x, z, own, :] for k in range(ITERS)]

            def combine(c, v):
                total = c[0] * v[0]
                for a, b in zip(c[1:], v[1:]):
                    total = total + a * b
                return total

            for z in range(parts):
                line = base[i, z] if turn < STEPS else None
                if with_p:
                    v = basis(0, z)
                    rise = combine(coeff[0][0], v)
                    change = combine(coeff[0][1], v)
                    before = p0[x, z, own, :] if turn == 0 else sums[0, i, z]
                    if turn + 1 < STEPS:
                        sums[0, i, z] = before + rise
                        heads_p[turn + 1, x, z, own, :] = v[0] - change
                    else:
                        result[0, i, z] = before + rise
                if with_c:
                    v = basis(len(fields) - 1, z)
                    rise = combine(coeff[-1][0], v)
                    before = p0[x, z, own, :] if turn == 1 else sums[1, i, z]
                    if turn < STEPS:
                        sums[1, i, z] = before + rise
                        line = line - combine(coeff[-1][1], v)
                        base[i, z] = line
                    else:
                        result[1, i, z] = before + rise
                if turn < STEPS:
                    heads_c[turn, x, z, own, :] = line + 0.5 * change
            return carry

        lax.fori_loop(0, half, update, 0)

    ends = []
    for other in range(1, levels):
        to = lax.rem(level + other, levels)
        for z in range(parts):
            lanes = slice(z * LANES, (z + 1) * LANES)
            copy = pltpu.make_async_remote_copy(
                src_ref=result.at[to, :, z, :, :], dst_ref=out_ref.at[0, mine, :, lanes],
                send_sem=out_sem.at[0, z], recv_sem=out_sem.at[1, z],
                device_id={"level": to, "gx": gx, "yz": yz}, device_id_type=MESH)
            copy.start()
            ends.append(copy)
    for z in range(parts):
        lanes = slice(z * LANES, (z + 1) * LANES)
        copy = pltpu.make_async_copy(result.at[level, :, z, :, :], out_ref.at[0, mine, :, lanes], out_sem.at[2, z])
        copy.start()
        ends.append(copy)
    for item in pending:
        end_halo(*item)
    for copy in ends:
        copy.wait()


def solution(mesh):
    levels, nx, ny = mesh.shape["level"], mesh.shape["gx"], mesh.shape["yz"]
    if levels * nx * ny <= 64:
        stages = (("level", "gx", "yz"),)
    else:
        stages = (("level", "gx"), ("yz",))

    def per_device(init_field, source, damping):
        deep, rows, wide = init_field.shape
        half, parts = deep // levels, wide // LANES
        padded = (half + 2 * PX, parts, rows + 2 * PY, LANES)
        plain = (half, parts, rows, LANES)
        counts = []
        for axes in stages:
            n = 1
            for a in axes:
                n *= mesh.shape[a]
            counts.append(n)
        turns = STEPS + 1
        dma = pltpu.SemaphoreType.DMA
        exchanges = 2 + 2 * STEPS
        return pl.pallas_call(
            functools.partial(body, (levels, nx, ny), stages),
            out_shape=jax.ShapeDtypeStruct((1, deep, rows, wide), jnp.float32),
            in_specs=[pl.BlockSpec(memory_space=pl.ANY)] * 3,
            out_specs=pl.BlockSpec(memory_space=pl.ANY),
            scratch_shapes=[
                pltpu.VMEM(padded, jnp.float32),
                pltpu.VMEM(plain, jnp.float32),
                pltpu.VMEM(padded, jnp.float32),
                pltpu.VMEM((STEPS,) + padded, jnp.float32),
                pltpu.VMEM((STEPS,) + padded, jnp.float32),
                pltpu.VMEM((ITERS,) + padded, jnp.float32),
                pltpu.VMEM((ITERS,) + padded, jnp.float32),
                pltpu.VMEM(plain, jnp.float32),
                pltpu.VMEM((2,) + plain, jnp.float32),
                pltpu.VMEM((2,) + plain, jnp.float32),
                [pltpu.VMEM((turns, n, LANES), jnp.float32) for n in counts],
                dma((3, parts)),
                dma((exchanges, 8)),
                dma((exchanges, 8)),
                [dma((turns, n - 1)) for n in counts],
                [dma((turns, n - 1)) for n in counts],
                dma((3, parts)),
            ],
            compiler_params=pltpu.CompilerParams(has_side_effects=True),
        )(init_field, source, damping)

    spec = P("gx", "yz", None)
    return jax.shard_map(
        per_device, mesh=mesh, in_specs=(spec, spec, spec),
        out_specs=P("level", "gx", "yz", None), check_vma=False,
    )
```

```python
import functools

import jax
import jax.numpy as jnp
from jax import lax
from jax.experimental import pallas as pl
from jax.experimental.pallas import tpu as pltpu
from jax.sharding import PartitionSpec as P

STEPS = 3
ITERS = 3
PX = 3
PY = 8
LANES = 128
MID = 8.025
HALF = 6.975
MESH = pl.DeviceIdType.MESH
DIRS = ((-1, 0), (1, 0), (0, -1), (0, 1), (-1, -1), (-1, 1), (1, -1), (1, 1))


def times_a(c):
    out = [MID * v for v in c] + [jnp.zeros_like(c[0])]
    for k, v in enumerate(c):
        if k == 0:
            out[1] = out[1] + HALF * v
        else:
            out[k + 1] = out[k + 1] + (0.5 * HALF) * v
            out[k - 1] = out[k - 1] + (0.5 * HALF) * v
    return out


def plus(a, b):
    short, long = (a, b) if len(a) < len(b) else (b, a)
    return [x + y for x, y in zip(short, long)] + long[len(short):]


def scaled(s, a):
    return [s * x for x in a]


def cg_coefficients(dots):
    m = [dots[0], dots[1], 2.0 * dots[2] - dots[0], 2.0 * dots[3] - dots[1],
         2.0 * dots[4] - dots[0], 2.0 * dots[5] - dots[1]]

    def inner(a, b):
        total = None
        for i, x in enumerate(a):
            for j, y in enumerate(b):
                term = (x * y) * (0.5 * (m[i + j] + m[abs(i - j)]))
                total = term if total is None else total + term
        return total

    one = jnp.ones_like(m[0])
    resid = [one]
    direction = resid
    image = times_a(resid)
    along = image
    norm_now = m[0]
    alpha = norm_now / inner(resid, image)
    answer = None
    for step in range(ITERS):
        move = scaled(alpha, direction)
        answer = move if answer is None else plus(answer, move)
        if step + 1 < ITERS:
            resid = plus(resid, scaled(-alpha, along))
            image = times_a(resid)
            norm_next = inner(resid, resid)
            product = inner(resid, image)
            ratio = norm_next / norm_now
            alpha = norm_next / (product - ratio * norm_next / alpha)
            direction = plus(resid, scaled(ratio, direction))
            along = plus(image, scaled(ratio, along))
            norm_now = norm_next
    change = plus(times_a(answer), scaled(-1.0, answer))
    return answer, change


def body(sizes, stages, init_ref, source_ref, damp_ref, out_ref, p0, src, dmp, heads_p, heads_c,
         work_p, work_c, ahead, base, sums, result, inbox, slots, in_sem, send_sem, recv_sem, red_send, red_recv, out_sem):
    levels, nx, ny = sizes
    half = src.shape[0]
    parts = src.shape[1]
    rows = src.shape[2]
    level, gx, yz = lax.axis_index("level"), lax.axis_index("gx"), lax.axis_index("yz")
    xpos = gx * levels + level
    xcount = nx * levels
    x_in = (xpos > 0, xpos < xcount - 1)
    y_in = (yz > 0, yz < ny - 1)

    def exists(dx, dy):
        ok = None
        for d, pair in ((dx, x_in), (dy, y_in)):
            if d != 0:
                c = pair[0] if d < 0 else pair[1]
                ok = c if ok is None else jnp.logical_and(ok, c)
        return ok

    mine = pl.ds(level * half, half)
    loads = []
    for i, (ref, buf, pad) in enumerate(((init_ref, p0, True), (damp_ref, dmp, True), (source_ref, src, False))):
        for z in range(parts):
            lanes = slice(z * LANES, (z + 1) * LANES)
            dst = buf.at[PX:PX + half, z, PY:PY + rows, :] if pad else buf.at[:, z, :, :]
            copy = pltpu.make_async_copy(ref.at[mine, :, lanes], dst, in_sem.at[i, z])
            copy.start()
            loads.append(copy)

    zero_x = jnp.zeros((PX,) + tuple(p0.shape[1:]), jnp.float32)
    zero_y = jnp.zeros((p0.shape[0], parts, PY, LANES), jnp.float32)
    for buf in [p0] + [h.at[n] for h in (heads_p, heads_c) for n in range(STEPS)]:
        @pl.when(jnp.logical_not(x_in[0]))
        def _(buf=buf):
            buf[0:PX] = zero_x

        @pl.when(jnp.logical_not(x_in[1]))
        def _(buf=buf):
            buf[PX + half:] = zero_x

        @pl.when(jnp.logical_not(y_in[0]))
        def _(buf=buf):
            buf[:, :, 0:PY, :] = zero_y

        @pl.when(jnp.logical_not(y_in[1]))
        def _(buf=buf):
            buf[:, :, PY + rows:, :] = zero_y

    def halo_copy(buf, width, slot, k, into=None):
        dx, dy = DIRS[k]
        w = width if 0 in (dx, dy) else width - 1
        if w == 0:
            return None

        def spans(d, pad, size):
            if d == 0:
                return slice(pad, pad + size), slice(pad, pad + size)
            if d < 0:
                return slice(pad, pad + w), slice(pad + size, pad + size + w)
            return slice(pad + size - w, pad + size), slice(pad - w, pad)

        sx, tx = spans(dx, PX, half)
        sy, ty = spans(dy, PY, rows)
        to = xpos + dx
        return pltpu.make_async_remote_copy(
            src_ref=buf.at[sx, :, sy, :], dst_ref=(buf if into is None else into).at[tx, :, ty, :],
            send_sem=send_sem.at[slot, k], recv_sem=recv_sem.at[slot, k],
            device_id={"level": lax.rem(to + levels, levels), "gx": lax.div(to + levels, levels) - 1, "yz": yz + dy},
            device_id_type=MESH,
        )

    order = (4, 5, 6, 7, 2, 3, 0, 1)

    def send_halo(buf, width, slot, into=None):
        for k in order:
            copy = halo_copy(buf, width, slot, k, into)
            if copy is not None:
                pl.when(exists(*DIRS[k]))(lambda copy=copy: copy.start())

    def wait_halo(buf, width, slot, into=None):
        for k in order:
            copy = halo_copy(buf, width, slot, k, into)
            if copy is not None:
                dx, dy = DIRS[k]
                pl.when(exists(-dx, -dy))(lambda copy=copy: copy.wait_recv())

    def end_halo(buf, width, slot, into=None):
        for k in order:
            copy = halo_copy(buf, width, slot, k, into)
            if copy is not None:
                pl.when(exists(*DIRS[k]))(lambda copy=copy: copy.wait_send())

    def stencil(v, x, start, count):
        lane = lax.broadcasted_iota(jnp.int32, (count, LANES), 1)
        own = pl.ds(start, count)
        centre = [v[x, z, own, :] for z in range(parts)]
        fore = [pltpu.roll(c, 1, 1) for c in centre]
        back = [pltpu.roll(c, LANES - 1, 1) for c in centre]
        out = []
        for z in range(parts):
            near = jnp.where(lane == 0, fore[z - 1] if z > 0 else 0.0, fore[z])
            far = jnp.where(lane == LANES - 1, back[z + 1] if z + 1 < parts else 0.0, back[z])
            beside = v[x - 1, z, own, :] + v[x + 1, z, own, :]
            beside = beside + v[x, z, pl.ds(start - 1, count), :] + v[x, z, pl.ds(start + 1, count), :]
            beside = beside + (near + far)
            out.append((dmp[x, z, own, :] + (7.0 - MID)) * centre[z] - beside)
        return out, centre

    low = jnp.where(y_in[0], 0, PY)
    high = jnp.where(y_in[1], 2 * PY + rows, PY + rows)

    def fold(block):
        return jnp.sum(block.reshape(-1, 8, LANES), axis=0)

    def powers(head, work):
        zero = jnp.zeros((8, LANES), jnp.float32)
        own = pl.ds(PY, rows)
        totals = []
        for k in range(1, ITERS + 1):
            h = ITERS - k
            start = PY - h
            count = -(-(rows + 2 * h) // 8) * 8
            prev = head if k == 1 else work.at[k - 2]
            row = lax.broadcasted_iota(jnp.int32, (count, LANES), 0) + start

            mask = jnp.logical_and(row >= low, row < high)
            keep = jnp.logical_and(row >= PY, row < PY + rows)
            older = None if k == 1 else head if k == 2 else work.at[k - 3]

            def plane(x, inner, sides, k=k, h=h, start=start, count=count, prev=prev, mask=mask, keep=keep, older=older):
                a, b = sides
                t, centre = stencil(prev, x, start, count)
                ok = mask
                if not inner:
                    ok = jnp.logical_and(mask, x_in[0] if x < PX else x_in[1])
                for z in range(parts):
                    if k == 1:
                        new = t[z] * (1.0 / HALF)
                    else:
                        new = t[z] * (2.0 / HALF) - older[x, z, pl.ds(start, count), :]
                    if h > 0:
                        new = jnp.where(ok, new, 0.0)
                    work[k - 1, x, z, pl.ds(start, count), :] = new
                    if inner:
                        square, cross = centre[z] * centre[z], centre[z] * new
                        if h > 0:
                            square, cross = jnp.where(keep, square, 0.0), jnp.where(keep, cross, 0.0)
                        a = a + fold(square)
                        b = b + fold(cross)
                return a, b

            sides = (zero, zero)
            for x in range(PX - h, PX + half + h):
                sides = plane(x, PX <= x < PX + half, sides)
            totals += sides
        return totals

    def position(axes):
        flat = 0
        for a in axes:
            flat = flat * lax.axis_size(a) + lax.axis_index(a)
        return flat

    def reduce_all(accs, turn, meanwhile):
        n = len(accs)
        size = -(-n // 8) * 8
        eye = lax.broadcasted_iota(jnp.int32, (size, LANES), 0) == lax.broadcasted_iota(jnp.int32, (size, LANES), 1)
        tall = jnp.concatenate([jnp.sum(a, axis=0, keepdims=True) for a in accs]
                               + [jnp.zeros((size - n, LANES), jnp.float32)] * (size > n), axis=0)
        col = jnp.sum(tall, axis=1, keepdims=True)
        line = jnp.sum(jnp.where(eye, col, 0.0), axis=0, keepdims=True)
        for s, axes in enumerate(stages):
            count = 1
            for a in axes:
                count *= lax.axis_size(a)
            me = position(axes)
            cell = slots[s].at[turn, pl.ds(me, 1), :]
            cell[...] = line
            copies = []
            for off in range(1, count):
                peer = lax.rem(me + off, count)
                ids = {}
                for a in reversed(axes):
                    ids[a] = lax.rem(peer, lax.axis_size(a))
                    peer = lax.div(peer, lax.axis_size(a))
                copy = pltpu.make_async_remote_copy(
                    src_ref=cell, dst_ref=cell, send_sem=red_send[s].at[turn, off - 1],
                    recv_sem=red_recv[s].at[turn, off - 1], device_id=ids, device_id_type=MESH)
                copy.start()
                copies.append(copy)
            if s == 0:
                for item in meanwhile:
                    send_halo(*item)
            for copy in copies:
                copy.wait_recv()
            line = jnp.sum(slots[s][turn], axis=0, keepdims=True)
            for copy in copies:
                copy.wait_send()
        col = jnp.sum(jnp.where(eye, line, 0.0), axis=1, keepdims=True)
        wide = jnp.broadcast_to(col, (size, LANES))
        return [wide[k:k + 1, :] for k in range(n)]

    def to_out(block, part, row):
        return [pltpu.make_async_copy(
            block.at[:, z, :, :], out_ref.at[0, pl.ds(part * half, half), :, slice(z * LANES, (z + 1) * LANES)],
            out_sem.at[row, z]) for z in range(parts)]

    def pieces(f):
        return to_out(result.at[f], level, 2)

    def across(f):
        return pltpu.make_async_remote_copy(
            src_ref=result.at[f], dst_ref=inbox, send_sem=out_sem.at[0, 0], recv_sem=out_sem.at[1, 0],
            device_id={"level": f, "gx": gx, "yz": yz}, device_id_type=MESH)

    def deliver(f):
        pl.when(level != f)(lambda: across(f).start())
        for copy in pieces(f):
            pl.when(level == f)(lambda copy=copy: copy.start())

    own = pl.ds(PY, rows)
    for copy in loads[:2 * parts]:
        copy.wait()
    send_halo(p0, 1, 0)
    send_halo(dmp, ITERS - 1, 1)
    for copy in loads[2 * parts:]:
        copy.wait()
    wait_halo(p0, 1, 0)

    def start_plane(x, carry):
        t, centre = stencil(p0, x, PY, rows)
        for z in range(parts):
            r = src[x - PX, z] - (t[z] + (MID - 1.0) * centre[z])
            heads_p[0, x, z, own, :] = r
            base[x - PX, z] = r
        return carry

    lax.fori_loop(PX, PX + half, start_plane, 0, unroll=True)

    pending = [(p0, 1, 0), (dmp, ITERS - 1, 1)]
    slot = 2
    for turn in range(STEPS + 1):
        with_p, with_c = turn < STEPS, turn > 0
        fields = []
        if with_p:
            fields.append((heads_p.at[turn], work_p))
        if with_c:
            fields.append((heads_c.at[turn - 1], work_c))
        slots_here = []
        for head, _ in fields:
            if turn != 1:
                send_halo(head, ITERS, slot)
                slots_here.append((head, ITERS, slot))
                slot += 1
        if turn == 0:
            wait_halo(dmp, ITERS - 1, 1)
        accs = []
        for i, (head, work) in enumerate(fields):
            if turn != 1:
                wait_halo(*slots_here[i])
            accs += powers(head, work)
        pending += slots_here
        outer = []
        if turn == 0:
            for k in range(ITERS):
                outer.append((work_p.at[k], ITERS, slot, ahead.at[k]))
                slot += 1
            pending += outer
        dots = reduce_all(accs, turn, outer)
        coeff = [cg_coefficients(dots[6 * i:6 * i + 6]) for i in range(len(fields))]

        def update(i, carry, turn=turn, with_p=with_p, with_c=with_c, fields=fields, coeff=coeff):
            x = i + PX

            def basis(f, z):
                head, work = fields[f]
                return [head[x, z, own, :]] + [work[k, x, z, own, :] for k in range(ITERS)]

            def combine(c, v):
                total = c[0] * v[0]
                for a, b in zip(c[1:], v[1:]):
                    total = total + a * b
                return total

            for z in range(parts):
                line = base[i, z] if turn < STEPS else None
                if with_p:
                    v = basis(0, z)
                    rise = combine(coeff[0][0], v)
                    change = combine(coeff[0][1], v)
                    before = p0[x, z, own, :] if turn == 0 else sums[0, i, z]
                    if turn + 1 < STEPS:
                        sums[0, i, z] = before + rise
                        heads_p[turn + 1, x, z, own, :] = v[0] - change
                    else:
                        result[0, i, z] = before + rise
                if with_c:
                    v = basis(len(fields) - 1, z)
                    rise = combine(coeff[-1][0], v)
                    before = p0[x, z, own, :] if turn == 1 else sums[1, i, z]
                    if turn < STEPS:
                        sums[1, i, z] = before + rise
                        line = line - combine(coeff[-1][1], v)
                        base[i, z] = line
                    else:
                        result[1, i, z] = before + rise
                if turn < STEPS:
                    heads_c[turn, x, z, own, :] = line + 0.5 * change
            return carry

        lax.fori_loop(0, half, update, 0, unroll=True)
        if turn == 0:
            for item in outer:
                wait_halo(*item)
                end_halo(*item)
            pending = pending[:-len(outer)]

            def rim(x, begin, count, plane_ok):
                span = pl.ds(begin, count)
                row = lax.broadcasted_iota(jnp.int32, (count, LANES), 0) + begin
                ok = jnp.logical_and(row >= low, row < high)
                if plane_ok is not None:
                    ok = jnp.logical_and(ok, plane_ok)
                for z in range(parts):
                    now = heads_p[0, x, z, span, :]
                    change = coeff[0][1][0] * now
                    for k in range(ITERS):
                        change = change + coeff[0][1][k + 1] * ahead[k, x, z, span, :]
                    heads_p[1, x, z, span, :] = jnp.where(ok, now - change, 0.0)
                    heads_c[0, x, z, span, :] = jnp.where(ok, now + 0.5 * change, 0.0)

            for x in range(PX):
                rim(x, 0, 2 * PY + rows, x_in[0])
                rim(PX + half + x, 0, 2 * PY + rows, x_in[1])
            for x in range(PX, PX + half):
                rim(x, 0, PY, None)
                rim(x, PY + rows, PY, None)
        if turn == STEPS - 1:
            deliver(0)
    deliver(1)

    for item in pending:
        end_halo(*item)
    for f in range(2):
        pl.when(level != f)(lambda f=f: across(f).wait_send())
        pl.when(level == f)(lambda f=f: across(f).wait_recv())
        for copy in pieces(f):
            pl.when(level == f)(lambda copy=copy: copy.wait())
    ends = to_out(inbox, 1 - level, 3)
    for copy in ends:
        copy.start()
    for copy in ends:
        copy.wait()


def solution(mesh):
    levels, nx, ny = mesh.shape["level"], mesh.shape["gx"], mesh.shape["yz"]
    if levels * nx * ny <= 64:
        stages = (("level", "gx", "yz"),)
    else:
        stages = (("level", "gx"), ("yz",))

    def per_device(init_field, source, damping):
        deep, rows, wide = init_field.shape
        half, parts = deep // levels, wide // LANES
        padded = (half + 2 * PX, parts, rows + 2 * PY, LANES)
        plain = (half, parts, rows, LANES)
        counts = []
        for axes in stages:
            n = 1
            for a in axes:
                n *= mesh.shape[a]
            counts.append(n)
        turns = STEPS + 1
        dma = pltpu.SemaphoreType.DMA
        exchanges = 2 + 2 * STEPS + ITERS
        return pl.pallas_call(
            functools.partial(body, (levels, nx, ny), stages),
            out_shape=jax.ShapeDtypeStruct((1, deep, rows, wide), jnp.float32),
            in_specs=[pl.BlockSpec(memory_space=pl.ANY)] * 3,
            out_specs=pl.BlockSpec(memory_space=pl.ANY),
            scratch_shapes=[
                pltpu.VMEM(padded, jnp.float32),
                pltpu.VMEM(plain, jnp.float32),
                pltpu.VMEM(padded, jnp.float32),
                pltpu.VMEM((STEPS,) + padded, jnp.float32),
                pltpu.VMEM((STEPS,) + padded, jnp.float32),
                pltpu.VMEM((ITERS,) + padded, jnp.float32),
                pltpu.VMEM((ITERS,) + padded, jnp.float32),
                pltpu.VMEM((ITERS,) + padded, jnp.float32),
                pltpu.VMEM(plain, jnp.float32),
                pltpu.VMEM((2,) + plain, jnp.float32),
                pltpu.VMEM((2,) + plain, jnp.float32),
                pltpu.VMEM(plain, jnp.float32),
                [pltpu.VMEM((turns, n, LANES), jnp.float32) for n in counts],
                dma((3, parts)),
                dma((exchanges, 8)),
                dma((exchanges, 8)),
                [dma((turns, n - 1)) for n in counts],
                [dma((turns, n - 1)) for n in counts],
                dma((4, parts)),
            ],
            compiler_params=pltpu.CompilerParams(has_side_effects=True),
        )(init_field, source, damping)

    spec = P("gx", "yz", None)
    return jax.shard_map(
        per_device, mesh=mesh, in_specs=(spec, spec, spec),
        out_specs=P("level", "gx", "yz", None), check_vma=False,
    )
```
